32 devices in a mesh: gx: 4 (over y, x), gy: 8 (over z, core).
Axes of the slice: x: 2, y: 2, z: 4, core: 2. Of those that a mesh axis runs over, the one named last changes fastest.
Arguments:
- u_wind: float32 [60, 256, 1024], P(None, 'gx', 'gy'), may hold values from -6 to 6
- v_wind: float32 [60, 256, 1024], P(None, 'gx', 'gy'), may hold values from -6 to 6
- w_wind: float32 [60, 256, 1024], P(None, 'gx', 'gy'), may hold values from -3 to 3
- pressure: float32 [60, 256, 1024], P(None, 'gx', 'gy'), may hold values from -6 to 6
- vert_coef: float32 [256, 1024], P('gx', 'gy'), may hold values from 0.2 to 5
- we_slab: float32 [2, 3, 60, 5, 1024], P(None, None, None, None, ('gy', 'gx')), may hold values from -8 to 8
- sn_slab: float32 [2, 3, 60, 5, 256], P(None, None, None, None, ('gx', 'gy')), may hold values from -8 to 8
- relax_width: int32 [256, 1024], P('gx', 'gy'), may hold values from 2 to 5
Outputs:
- u_out: float32 [60, 256, 1024], P(None, 'gx', 'gy')
- v_out: float32 [60, 256, 1024], P(None, 'gx', 'gy')
- w_out: float32 [60, 256, 1024], P(None, 'gx', 'gy')
- p_out: float32 [60, 256, 1024], P(None, 'gx', 'gy')
The draws below stay inside these ranges and needn't reach their ends.
All inputs are finite; a program needn't handle non-finite values.
Results may differ from the reference program's by a relative error of at most 0.0001.
Values sent between devices are 32-bit elements; how exact they have to be, the bound alone decides.
A program may use at most 192 MiB of HBM per device.

```python
import math
import jax
import jax.numpy as jnp
from jax import lax

NZ = 60
W = 5
SUBSTEPS = 6
NX = 256
NY = 1024


def place_ends(drawn, stream_key, smallest, largest):
    shape = drawn.shape
    place = [jax.random.randint(jax.random.fold_in(stream_key, axis), (), 0, shape[axis]) for axis in range(len(shape))]
    drawn = drawn.at[tuple(place)].set(smallest)
    longest = shape.index(max(shape))
    place[longest] = (place[longest] + 1) % shape[longest]
    return drawn.at[tuple(place)].set(largest)


def level_of(rng, shape, split, smallest, high):
    level = 1.0
    for position, blocks in split:
        draws = jax.random.uniform(jax.random.fold_in(jax.random.fold_in(rng, 6), position), (blocks,), jnp.float32, smallest / len(split), high / len(split))
        level = level * jnp.repeat(jnp.exp(draws), shape[position] // blocks).reshape((-1,) + (1,) * (len(shape) - 1 - position))
    return level


def normal_values(own_key, dims, deviation, bound, pieces=(), kind=jnp.bfloat16):
    array = deviation * jax.random.normal(own_key, dims, jnp.float32)
    if pieces:
        array = array * level_of(own_key, dims, pieces, -0.22, 0.18)
    return jnp.clip(array, -bound, bound).astype(kind)


def setup_inputs(seed: int = 0) -> dict:
    seeds = jax.random.split(jax.random.key(seed), 9)
    u_wind = normal_values(seeds[0], (NZ, NX, NY), 1.0, 6.0, ((1, 4), (2, 8)), jnp.float32)
    v_wind = normal_values(seeds[1], (NZ, NX, NY), 1.0, 6.0, ((1, 4), (2, 8)), jnp.float32)
    w_wind = normal_values(seeds[2], (NZ, NX, NY), 0.5, 3.0, ((1, 4), (2, 8)), jnp.float32)
    pressure = normal_values(seeds[3], (NZ, NX, NY), 1.0, 6.0, ((1, 4), (2, 8)), jnp.float32)
    vert_coef = jnp.clip(jnp.exp(math.log(5.0) - 3.218876 * jax.random.uniform(seeds[4], (NX, NY), jnp.float32) ** level_of(seeds[4], (NX, NY), ((0, 4), (1, 8)), -0.2, 0.2)), 0.2, 5.0)
    we_slab = normal_values(seeds[5], (2, 3, NZ, W, NY), 1.5, 8.0, ((4, 32),), jnp.float32)
    sn_slab = normal_values(seeds[6], (2, 3, NZ, W, NX), 1.5, 8.0, ((4, 32),), jnp.float32)
    relax_width = place_ends(jax.random.randint(seeds[7], (NX, NY), 2, W + 1), jax.random.fold_in(seeds[7], 1), 2, W).astype(jnp.int32)
    return dict(u_wind=u_wind, v_wind=v_wind, w_wind=w_wind, pressure=pressure, vert_coef=vert_coef, we_slab=we_slab, sn_slab=sn_slab, relax_width=relax_width)


accel = 0.3
spread = 0.3
buoyancy = 0.5


def tri_solve(coef, rhs):
    def forward(carry, item):
        prev_c, prev_d = carry
        denom = 1.0 + 2.0 * coef + coef * prev_c
        next_c = -coef / denom
        next_d = (item + coef * prev_d) / denom
        return (next_c, next_d), (next_c, next_d)

    zero = jnp.zeros_like(coef)
    _, (cees, dees) = lax.scan(forward, (zero, zero), rhs)

    def backward(above, item):
        c_here, d_here = item
        value = d_here - c_here * above
        return value, value

    _, solved = lax.scan(backward, zero, (cees, dees), reverse=True)
    return solved


def blend(field, rows_k, cols_k, xpos, ypos, nx_total, ny_total, rate):
    band = rows_k.shape[2]
    size_x = field.shape[1]
    size_y = field.shape[2]
    west = jnp.pad(rows_k[0], ((0, 0), (0, size_x - band), (0, 0)))
    east = jnp.pad(rows_k[1][:, ::-1, :], ((0, 0), (size_x - band, 0), (0, 0)))
    south = jnp.pad(jnp.transpose(cols_k[0], (0, 2, 1)), ((0, 0), (0, 0), (0, size_y - band)))
    north = jnp.pad(jnp.transpose(cols_k[1][:, ::-1, :], (0, 2, 1)), ((0, 0), (0, 0), (size_y - band, 0)))
    weight_w = jnp.maximum(rate - xpos[:, None], 0.0) / rate
    weight_e = jnp.maximum(rate - (nx_total - 1.0 - xpos)[:, None], 0.0) / rate
    weight_s = jnp.maximum(rate - ypos[None, :], 0.0) / rate
    weight_n = jnp.maximum(rate - (ny_total - 1.0 - ypos)[None, :], 0.0) / rate
    field = field + weight_w[None] * (west - field)
    field = field + weight_e[None] * (east - field)
    field = field + weight_s[None] * (south - field)
    field = field + weight_n[None] * (north - field)
    return field


def column_part(u_new, v_new, west_u, south_v, w_old, p_old, coef):
    diverge = (u_new - west_u) + (v_new - south_v)
    sectioned = p_old - spread * diverge
    above_q = jnp.concatenate([sectioned[1:], jnp.zeros_like(sectioned[:1])], axis=0)
    rhs = w_old + buoyancy * (sectioned - above_q)
    w_new = tri_solve(coef, rhs)
    below_w = jnp.concatenate([jnp.zeros_like(w_new[:1]), w_new[:-1]], axis=0)
    p_new = sectioned - buoyancy * (w_new - below_w)
    return w_new, p_new


def reference(u_wind, v_wind, w_wind, pressure, vert_coef, we_slab, sn_slab, relax_width):
    size_x = pressure.shape[1]
    size_y = pressure.shape[2]
    xpos = jnp.arange(size_x, dtype=jnp.int32).astype(jnp.float32)
    ypos = jnp.arange(size_y, dtype=jnp.int32).astype(jnp.float32)
    rate = relax_width.astype(jnp.float32)
    fields = []
    for index, field in enumerate((u_wind, v_wind, pressure)):
        fields.append(blend(field, we_slab[:, index], sn_slab[:, index], xpos, ypos, float(size_x), float(size_y), rate))
    u_now, v_now, p_now = fields
    w_now = w_wind
    for step in range(SUBSTEPS):
        east_p = jnp.concatenate([p_now[:, 1:, :], jnp.zeros_like(p_now[:, :1, :])], axis=1)
        north_p = jnp.concatenate([p_now[:, :, 1:], jnp.zeros_like(p_now[:, :, :1])], axis=2)
        u_now = u_now - accel * (east_p - p_now)
        v_now = v_now - accel * (north_p - p_now)
        west_u = jnp.concatenate([jnp.zeros_like(u_now[:, :1, :]), u_now[:, :-1, :]], axis=1)
        south_v = jnp.concatenate([jnp.zeros_like(v_now[:, :, :1]), v_now[:, :, :-1]], axis=2)
        w_now, p_now = column_part(u_now, v_now, west_u, south_v, w_now, p_now, vert_coef)
    return u_now, v_now, w_now, p_now
```

```python
import jax
import jax.numpy as jnp
from jax import lax
from jax.experimental import pallas as pl
from jax.experimental.pallas import tpu as pltpu
from jax.sharding import PartitionSpec as P

SUBSTEPS = 6
ACCEL = 0.3
SPREAD = 0.3
BUOYANCY = 0.5
LANES = 128
ROWS = 16
PAD = 8
UNROLL = 4


def make_kernel(levels, size_x, size_y, groups):
    blocks = size_x // ROWS
    order = [0, blocks - 1] + list(range(1, blocks - 1))
    per_group = levels // groups

    def kernel(u_hbm, v_hbm, w_hbm, p_hbm, coef, width, we_val, sn_val,
               u_out, v_out, w_out, p_out,
               U, V, W, D, M, S, rinv_ref, q_ref, e_ref,
               pack, recv_s, recv_n, vpack, vrecv,
               load_sem, out_sem, send_s, send_n, send_w, send_e,
               rs_sem, rn_sem, rw_sem, re_sem, us_sem, ur_sem, vs_sem, vr_sem):
        gx, gy = lax.axis_index("gx"), lax.axis_index("gy")
        nx, ny = lax.axis_size("gx"), lax.axis_size("gy")
        has_w, has_e = gx > 0, gx < nx - 1
        has_s, has_n = gy > 0, gy < ny - 1

        def rows(b):
            return pl.ds(PAD + b * ROWS, ROWS)

        loads = {}
        for b in order:
            for i, (src, dst) in enumerate(((u_hbm, U), (v_hbm, V), (p_hbm, S.at[0]))):
                loads[b, i] = pltpu.make_async_copy(
                    src.at[:, pl.ds(b * ROWS, ROWS), :], dst.at[:, rows(b), :], load_sem.at[i * blocks + b])
                loads[b, i].start()
        load_w = pltpu.make_async_copy(w_hbm, W, load_sem.at[3 * blocks])
        load_w.start()

        zero_rows = jnp.zeros((levels, PAD, size_y), jnp.float32)
        for par in range(2):
            S[par, :, :PAD, :] = zero_rows
            S[par, :, PAD + size_x:, :] = zero_rows
        U[:, :PAD, :] = zero_rows
        recv_s[...] = jnp.zeros(recv_s.shape, jnp.float32)
        recv_n[...] = jnp.zeros(recv_n.shape, jnp.float32)
        vrecv[...] = jnp.zeros(vrecv.shape, jnp.float32)

        barrier = pltpu.get_barrier_semaphore()
        sides = ((has_w, "gx", gx - 1), (has_e, "gx", gx + 1), (has_s, "gy", gy - 1), (has_n, "gy", gy + 1))
        for cond, axis, dev in sides:
            @pl.when(cond)
            def _(axis=axis, dev=dev):
                pl.semaphore_signal(barrier, inc=1, device_id={axis: dev}, device_id_type=pl.DeviceIdType.MESH)

        rinv = 1.0 / coef[...]
        rinv_ref[...] = rinv
        kappa = 2.0 + rinv

        def factor(z, m):
            m = 1.0 / (kappa - m)
            M[z] = m
            return m

        lax.fori_loop(0, levels, factor, jnp.zeros_like(kappa))
        S[1, :, pl.ds(PAD, size_x), :] = jnp.zeros((levels, size_x, size_y), jnp.float32)

        peers = (jnp.int32(4) - (gx == 0).astype(jnp.int32) - (gx == nx - 1).astype(jnp.int32)
                 - (gy == 0).astype(jnp.int32) - (gy == ny - 1).astype(jnp.int32))
        pl.semaphore_wait(barrier, peers)

        def remote(src, dst, ss, rs, axis, dev):
            return pltpu.make_async_remote_copy(
                src_ref=src, dst_ref=dst, send_sem=ss, recv_sem=rs,
                device_id={axis: dev}, device_id_type=pl.DeviceIdType.MESH)

        def to_south(par, b):
            return remote(pack.at[b], recv_n.at[par, b], send_s.at[b], rn_sem.at[par, b], "gy", gy - 1)

        def to_north(par, b):
            return remote(pack.at[b], recv_s.at[par, b], send_n.at[b], rs_sem.at[par, b], "gy", gy + 1)

        def to_west(par):
            return remote(S.at[par, :, pl.ds(PAD, 1), :], S.at[par, :, pl.ds(PAD + size_x, 1), :],
                          send_w.at[par], re_sem.at[par], "gx", gx - 1)

        def to_east(par):
            return remote(S.at[par, :, pl.ds(PAD + size_x - 1, 1), :], S.at[par, :, pl.ds(PAD - 1, 1), :],
                          send_e.at[par], rw_sem.at[par], "gx", gx + 1)

        def u_east():
            return remote(U.at[:, pl.ds(PAD + size_x - 1, 1), :], U.at[:, pl.ds(PAD - 1, 1), :],
                          us_sem, ur_sem, "gx", gx + 1)

        def v_north(b):
            return remote(vpack.at[b], vrecv.at[b], vs_sem.at[b], vr_sem.at[b], "gy", gy + 1)

        def send_block(par, b):
            @pl.when(has_s)
            def _():
                to_south(par, b).start()

            @pl.when(jnp.logical_not(has_s))
            def _():
                recv_s[par, b] = pltpu.roll(pack[b], LANES - 1, 1)

            @pl.when(has_n)
            def _():
                to_north(par, b).start()

            if b == 0:
                @pl.when(has_w)
                def _():
                    to_west(par).start()

                @pl.when(jnp.logical_not(has_w))
                def _():
                    S[par, :, PAD - 1:PAD, :] = S[par, :, PAD:PAD + 1, :]
            if b == blocks - 1:
                @pl.when(has_e)
                def _():
                    to_east(par).start()

        def wait_sent(par, b):
            @pl.when(has_s)
            def _():
                to_south(par, b).wait_send()

            @pl.when(has_n)
            def _():
                to_north(par, b).wait_send()

            if b == 0:
                @pl.when(has_w)
                def _():
                    to_west(par).wait_send()
            if b == blocks - 1:
                @pl.when(has_e)
                def _():
                    to_east(par).wait_send()

        def wait_halo(par, b):
            @pl.when(has_s)
            def _():
                to_north(par, b).wait_recv()

            @pl.when(has_n)
            def _():
                to_south(par, b).wait_recv()

            if b == 0:
                @pl.when(has_w)
                def _():
                    to_east(par).wait_recv()
            if b == blocks - 1:
                @pl.when(has_e)
                def _():
                    to_west(par).wait_recv()

        lane = lax.broadcasted_iota(jnp.int32, (ROWS, LANES), 1)
        half = lane // 2
        even = (lane % 2) == 0
        first, last = lane == 0, lane == LANES - 1

        rate = width[...].astype(jnp.float32)
        x_at = lax.broadcasted_iota(jnp.int32, rate.shape, 0) + gx * size_x
        y_at = lax.broadcasted_iota(jnp.int32, rate.shape, 1) + gy * size_y
        d_x = jnp.minimum(x_at, nx * size_x - 1 - x_at).astype(jnp.float32)
        d_y = jnp.minimum(y_at, ny * size_y - 1 - y_at).astype(jnp.float32)
        wgt_x = jnp.maximum(rate - d_x, 0.0) / rate
        wgt_y = jnp.maximum(rate - d_y, 0.0) / rate
        fields = (U, V, S.at[0])
        for b in order:
            for i in range(3):
                loads[b, i].wait()
            for is_here, cond, row in ((b == 0, jnp.logical_not(has_w), 0),
                                       (b == blocks - 1, jnp.logical_not(has_e), size_x - 8)):
                if is_here:
                    wx = wgt_x[row:row + 8]

                    @pl.when(cond)
                    def _(row=row, wx=wx):
                        def body(z, _):
                            for k, f in enumerate(fields):
                                at = pl.ds(PAD + row, 8)
                                old = f[z, at, :]
                                f[z, at, :] = old + wx * (we_val[k, z] - old)
                            return 0
                        lax.fori_loop(0, levels, body, 0, unroll=UNROLL)
            wy = wgt_y[b * ROWS:(b + 1) * ROWS]

            @pl.when(jnp.logical_not(jnp.logical_and(has_s, has_n)))
            def _(b=b, wy=wy):
                for g in range(groups):
                    def body(j, _, g=g):
                        z = g * per_group + j
                        for k, f in enumerate(fields):
                            old = f[z, rows(b), :]
                            val = pltpu.roll(sn_val[k, g, pl.ds(b * ROWS, ROWS), :], lax.rem(LANES - 5 * j, LANES), 1)
                            f[z, rows(b), :] = old + wy * (val - old)
                        return 0
                    lax.fori_loop(0, per_group, body, 0, unroll=UNROLL)

            def body(z, accs, b=b):
                acc, vacc = accs
                here = half == z
                acc = jnp.where(here, pltpu.roll(S[0, z, rows(b), :], 2 * z + 1, 1), acc)
                vacc = jnp.where(here, pltpu.roll(V[z, rows(b), :], 2 * z + 1, 1), vacc)
                return acc, vacc

            blank = jnp.zeros((ROWS, LANES), jnp.float32)
            acc, vacc = lax.fori_loop(0, levels, body, (blank, blank), unroll=UNROLL)
            pack[b] = acc
            vpack[b] = vacc
            send_block(0, b)

            @pl.when(has_n)
            def _(b=b):
                v_north(b).start()
            if b == blocks - 1:
                @pl.when(has_e)
                def _():
                    u_east().start()

        for b in order:
            @pl.when(has_s)
            def _(b=b):
                v_north(b).wait_recv()
            if b == 0:
                @pl.when(has_w)
                def _():
                    u_east().wait_recv()
            halo = vrecv[b]

            def body(z, _, b=b, halo=halo):
                v_here = V[z, rows(b), :]
                south = jnp.where(first, pltpu.roll(halo, lax.rem(LANES - 2 * z, LANES), 1), pltpu.roll(v_here, 1, 1))
                west = U[z, pl.ds(PAD - 1 + b * ROWS, ROWS), :]
                D[z, pl.ds(b * ROWS, ROWS), :] = SPREAD * ((U[z, rows(b), :] - west) + (v_here - south))
                return 0

            lax.fori_loop(0, levels, body, 0, unroll=UNROLL)
        load_w.wait()

        @pl.when(has_n)
        def _():
            for b in order:
                v_north(b).wait_send()

        @pl.when(has_e)
        def _():
            u_east().wait_send()

        out_copies = []

        def block_step(par, b, final):
            nxt = 1 - par
            at = pl.ds(b * ROWS, ROWS)
            wait_halo(par, b)
            mix = jnp.where(even, pltpu.roll(recv_n[par, b], LANES - 1, 1), pltpu.roll(recv_s[par, b], 1, 1))
            rin = rinv_ref[at, :]

            def calc_q(z):
                c = S[par, z, rows(b), :]
                west = S[par, z, pl.ds(PAD - 1 + b * ROWS, ROWS), :]
                east = S[par, z, pl.ds(PAD + 1 + b * ROWS, ROWS), :]
                rim = pltpu.roll(mix, LANES - 1 - 2 * z, 1)
                south = jnp.where(first, rim, pltpu.roll(c, 1, 1))
                north = jnp.where(last, rim, pltpu.roll(c, LANES - 1, 1))
                lap = ((west + east) + (south + north)) - 4.0 * c
                if final:
                    U[z, rows(b), :] = U[z, rows(b), :] - ACCEL * (east - c)
                    V[z, rows(b), :] = V[z, rows(b), :] - ACCEL * (north - c)
                return ((c - S[nxt, z, rows(b), :]) - D[z, at, :]) + (ACCEL * SPREAD) * lap

            def forward(z, carry, edge=False):
                d, q = carry
                q_up = jnp.zeros_like(q) if edge else calc_q(z + 1)
                e = (W[z, at, :] + BUOYANCY * (q - q_up)) * rin + d
                e_ref[z] = e
                q_ref[z] = q
                return M[z, at, :] * e, q_up

            carry = (jnp.zeros((ROWS, LANES), jnp.float32), calc_q(0))
            carry = lax.fori_loop(0, levels - 1, forward, carry, unroll=UNROLL)
            forward(levels - 1, carry, edge=True)
            wait_sent(par, b)

            def finish(z, w, below, acc):
                p = q_ref[z] - BUOYANCY * (w - below)
                if final:
                    S[nxt, z, rows(b), :] = p
                    return acc
                s = S[par, z, rows(b), :] + p
                S[nxt, z, rows(b), :] = s
                return jnp.where(half == z, pltpu.roll(s, 2 * z + 1, 1), acc)

            def backward(k, carry):
                z = levels - 2 - k
                w_up, acc = carry
                w = M[z, at, :] * (e_ref[z] + w_up)
                W[z, at, :] = w
                return w, finish(z + 1, w_up, w, acc)

            w_top = M[levels - 1, at, :] * e_ref[levels - 1]
            W[levels - 1, at, :] = w_top
            blank = jnp.zeros((ROWS, LANES), jnp.float32)
            w, acc = lax.fori_loop(0, levels - 1, backward, (w_top, blank), unroll=UNROLL)
            acc = finish(0, w, jnp.zeros_like(w), acc)
            if not final:
                pack[b] = acc
                send_block(nxt, b)
            else:
                for i, (src, dst, at_src) in enumerate(((U, u_out, rows(b)), (V, v_out, rows(b)),
                                                        (W, w_out, at), (S.at[nxt], p_out, rows(b)))):
                    copy = pltpu.make_async_copy(src.at[:, at_src, :], dst.at[:, at, :], out_sem.at[i * blocks + b])
                    copy.start()
                    out_copies.append(copy)

        def substep(step, _):
            for b in order:
                block_step(lax.rem(step, 2), b, False)
            return 0

        lax.fori_loop(0, SUBSTEPS - 1, substep, 0)
        for b in order:
            block_step((SUBSTEPS - 1) % 2, b, True)
        for copy in out_copies:
            copy.wait()

    return kernel


def per_device(u_wind, v_wind, w_wind, pressure, vert_coef, we_slab, sn_slab, relax_width):
    levels, size_x, size_y = pressure.shape
    band = we_slab.shape[3]
    groups = -(-levels * band // LANES)
    while levels % groups:
        groups += 1
    gx, gy = lax.axis_index("gx"), lax.axis_index("gy")
    edge = lax.all_gather(we_slab, "gx", axis=4, tiled=True)
    side = lax.all_gather(sn_slab, "gy", axis=4, tiled=True)
    none = (0, 0)
    we_val = jnp.where(gx == 0,
                       jnp.pad(edge[0], (none, none, (0, 8 - band), none)),
                       jnp.pad(edge[1][:, :, ::-1], (none, none, (8 - band, 0), none)))
    sn = jnp.where(gy == 0, side[0], side[1][:, :, ::-1])
    sn = sn.reshape(3, groups, levels // groups * band, size_x).transpose(0, 1, 3, 2)
    sn = jnp.pad(sn, (none, none, none, (0, LANES - sn.shape[3])))
    sn_val = jnp.where(gy == 0, sn, jnp.roll(sn, -band, axis=3))

    blocks = size_x // ROWS
    f32 = jnp.float32
    full = (levels, size_x, size_y)
    tall = (levels, size_x + 2 * PAD, size_y)
    any_spec = pl.BlockSpec(memory_space=pl.ANY)
    vmem_spec = pl.BlockSpec(memory_space=pltpu.VMEM)
    dma = pltpu.SemaphoreType.DMA
    return pl.pallas_call(
        make_kernel(levels, size_x, size_y, groups),
        out_shape=[jax.ShapeDtypeStruct(full, f32)] * 4,
        in_specs=[any_spec] * 4 + [vmem_spec] * 4,
        out_specs=[any_spec] * 4,
        scratch_shapes=[
            pltpu.VMEM(tall, f32), pltpu.VMEM(tall, f32), pltpu.VMEM(full, f32), pltpu.VMEM(full, f32),
            pltpu.VMEM(full, f32), pltpu.VMEM((2,) + tall, f32), pltpu.VMEM((size_x, size_y), f32),
            pltpu.VMEM((levels, ROWS, LANES), f32), pltpu.VMEM((levels, ROWS, LANES), f32),
            pltpu.VMEM((blocks, ROWS, LANES), f32), pltpu.VMEM((2, blocks, ROWS, LANES), f32),
            pltpu.VMEM((2, blocks, ROWS, LANES), f32), pltpu.VMEM((blocks, ROWS, LANES), f32),
            pltpu.VMEM((blocks, ROWS, LANES), f32),
            dma((3 * blocks + 1,)), dma((4 * blocks,)), dma((blocks,)), dma((blocks,)), dma((2,)), dma((2,)),
            dma((2, blocks)), dma((2, blocks)), dma((2,)), dma((2,)), dma, dma, dma((blocks,)), dma((blocks,)),
        ],
        compiler_params=pltpu.CompilerParams(collective_id=0, has_side_effects=True, vmem_limit_bytes=60 * 2**20),
    )(u_wind, v_wind, w_wind, pressure, vert_coef, relax_width, we_val, sn_val)


def solution(mesh):
    cells = P(None, "gx", "gy")
    return jax.shard_map(
        per_device,
        mesh=mesh,
        in_specs=(cells, cells, cells, cells, P("gx", "gy"),
                  P(None, None, None, None, ("gy", "gx")), P(None, None, None, None, ("gx", "gy")), P("gx", "gy")),
        out_specs=(cells,) * 4,
        check_vma=False,
    )
```
